32 devices in a mesh: fsdp: 4 (over z), ctx: 2 (over x), tp: 4 (over y, core).
Axes of the slice: x: 2, y: 2, z: 4, core: 2. Of those that a mesh axis runs over, the one named last changes fastest.
Arguments:
- block_input: bfloat16 [8192, 1536], P(('fsdp', 'ctx')), may hold values from -6 to 6
- seq_lengths: int32 [4, 4], P('fsdp'), may hold values from 1 to 1024, 2048 in all within a row
- attn_gain: bfloat16 [1536], P('fsdp'), may hold values from 0.099609375 to 1.8984375
- w_query: bfloat16 [1536, 1536], P('fsdp', 'tp')
- w_key: bfloat16 [1536, 768], P('fsdp', 'tp')
- value_weight: bfloat16 [1536, 768], P('fsdp', 'tp'), may hold values from -0.15625 to 0.15625
- w_out: bfloat16 [1536, 1536], P('tp', 'fsdp'), may hold values from -0.625 to 0.625
- mlp_gain: bfloat16 [1536], P('fsdp'), may hold values from 0.099609375 to 1.8984375
- w_gate: bfloat16 [1536, 4096], P('fsdp', 'tp'), may hold values from -0.15625 to 0.15625
- w_up: bfloat16 [1536, 4096], P('fsdp', 'tp'), may hold values from -0.15625 to 0.15625
- w_down: bfloat16 [4096, 1536], P('tp', 'fsdp'), may hold values from -0.09375 to 0.09375
- cotangent: bfloat16 [8192, 1536], P(('fsdp', 'ctx')), may hold values from -6 to 6
Outputs:
- block_output: bfloat16 [8192, 1536], P(('fsdp', 'ctx'))
- input_grad: float32 [8192, 1536], P(('fsdp', 'ctx'))
- attn_gain_grad: float32 [1536], P('fsdp')
- w_query_grad: float32 [1536, 1536], P('fsdp', 'tp')
- w_key_grad: float32 [1536, 768], P('fsdp', 'tp')
- w_value_grad: float32 [1536, 768], P('fsdp', 'tp')
- w_out_grad: float32 [1536, 1536], P('tp', 'fsdp')
- mlp_gain_grad: float32 [1536], P('fsdp')
- w_gate_grad: float32 [1536, 4096], P('fsdp', 'tp')
- w_up_grad: float32 [1536, 4096], P('fsdp', 'tp')
- w_down_grad: float32 [4096, 1536], P('tp', 'fsdp')
The draws below stay inside these ranges and needn't reach their ends.
Inputs may be any that keep to these rules, and one draw needn't show every extreme that they name: `seq_lengths`: row g lists the lengths of the 4 sequences of group g, laid end to end from its first token; each row sums to 2048 and its largest entry is exactly 1024.
All inputs are finite; a program needn't handle non-finite values.
Results may differ from the reference program's by a relative error of at most 0.028.
Values may be sent and summed in bfloat16 or wider, within the bound.
A program may use at most 192 MiB of HBM per device.

```python
import math
import jax
import jax.numpy as jnp
import numpy as np
from jax import lax

MODEL_WIDTH = 1536
QUERY_HEADS = 16
KEY_VALUE_HEADS = 8
HEAD_SIZE = 96
FF = 4096
NSEQ = 4
GROUP_TOK = 2048
SEQ_MAX = 1024
TOKENS = 8192
N_FSDP = 4


def draw_w_query(key, part):
    base_portion = jax.random.normal(jax.random.fold_in(key, 11), (MODEL_WIDTH, QUERY_HEADS * HEAD_SIZE), jnp.float32) / math.sqrt(MODEL_WIDTH)
    return base_portion.astype(jnp.bfloat16)


def draw_w_key(key, part):
    base_portion = jax.random.normal(jax.random.fold_in(key, 12), (MODEL_WIDTH, KEY_VALUE_HEADS * HEAD_SIZE), jnp.float32) / math.sqrt(MODEL_WIDTH)
    return base_portion.astype(jnp.bfloat16)


def block_levels(own_key, dims, pieces, smallest, high):
    loudness = 1.0
    for dim, parts in pieces:
        heights = jax.random.uniform(jax.random.fold_in(jax.random.fold_in(own_key, 6), dim), (parts,), jnp.float32, smallest / len(pieces), high / len(pieces))
        loudness = loudness * jnp.repeat(jnp.exp(heights), dims[dim] // parts).reshape((-1,) + (1,) * (len(dims) - 1 - dim))
    return loudness


def profile(count, total, limit, lean):
    loads = [(1 << 20) // math.isqrt(standing ** lean) + 1 for standing in range(2, count + 1)]
    surplus, counts = total - limit - (count - 1), [1] * (count - 1)
    while surplus > 0:
        free = [i for i in range(count - 1) if counts[i] < limit]
        whole, budget = sum([loads[i] for i in free]), surplus
        for i in free:
            more = min(limit - counts[i], max(1, budget * loads[i] // whole), surplus)
            counts[i] = counts[i] + more
            surplus = surplus - more
    return np.array([limit] + counts)


def uneven_parts(rng, number_of, total, limit, slope):
    if number_of == 2:
        one = jax.random.randint(rng, (), max(1, total - limit), min(limit, total - 1) + 1)
        return jnp.stack([one, total - one])
    tallies = jnp.asarray(profile(number_of, total, limit, slope), jnp.int32)
    pairs = (number_of - 1) // 2
    giver, receiver = tallies[1:1 + 2 * pairs:2], tallies[2:2 + 2 * pairs:2]
    room = jnp.minimum(giver - 1, limit - receiver)
    shifted = jax.random.randint(jax.random.fold_in(rng, 1), (pairs,), 0, 1 << 20) % (room + 1)
    tallies = tallies.at[1:1 + 2 * pairs:2].set(giver - shifted).at[2:2 + 2 * pairs:2].set(receiver + shifted)
    return tallies[jax.random.permutation(jax.random.fold_in(rng, 2), number_of)]


def gaussian(key, shape, width, most, shards=(), kind=jnp.bfloat16):
    drawn = width * jax.random.normal(key, shape, jnp.float32)
    if shards:
        drawn = drawn * block_levels(key, shape, shards, -0.22, 0.18)
    return jnp.clip(drawn, -most, most).astype(kind)


def setup_inputs(seed: int = 0) -> dict:
    key_list = jax.random.split(jax.random.key(seed), 13)
    block_input = gaussian(key_list[0], (TOKENS, MODEL_WIDTH), 1.0, 6.0, ((0, 8),))
    seq_lengths = jax.vmap(lambda own: uneven_parts(own, NSEQ, GROUP_TOK, SEQ_MAX, 2))(jax.random.split(key_list[1], N_FSDP)).reshape((N_FSDP, NSEQ)).astype(jnp.int32)
    attn_gain = jnp.clip(1.0 + 0.18 * jax.random.normal(key_list[2], (MODEL_WIDTH,), jnp.float32), 0.099609375, 1.8984375).astype(jnp.bfloat16)
    w_query = draw_w_query(jax.random.fold_in(key_list[12], 71), 0)
    w_key = draw_w_key(jax.random.fold_in(key_list[12], 71), 0)
    value_weight = gaussian(key_list[5], (MODEL_WIDTH, KEY_VALUE_HEADS * HEAD_SIZE), MODEL_WIDTH ** -0.5, 0.15625, ((0, 4), (1, 4)))
    w_out = gaussian(key_list[6], (QUERY_HEADS * HEAD_SIZE, MODEL_WIDTH), (QUERY_HEADS * HEAD_SIZE // 16) ** -0.5, 0.625, ((0, 4), (1, 4)))
    mlp_gain = jnp.clip(1.0 + 0.18 * jax.random.normal(key_list[7], (MODEL_WIDTH,), jnp.float32), 0.099609375, 1.8984375).astype(jnp.bfloat16)
    w_gate = gaussian(key_list[8], (MODEL_WIDTH, FF), MODEL_WIDTH ** -0.5, 0.15625, ((0, 4), (1, 4)))
    w_up = gaussian(key_list[9], (MODEL_WIDTH, FF), MODEL_WIDTH ** -0.5, 0.15625, ((0, 4), (1, 4)))
    w_down = gaussian(key_list[10], (FF, MODEL_WIDTH), FF ** -0.5, 0.09375, ((0, 4), (1, 4)))
    cotangent = gaussian(key_list[11], (TOKENS, MODEL_WIDTH), 1.0, 6.0, ((0, 8),))
    return dict(block_input=block_input, seq_lengths=seq_lengths, attn_gain=attn_gain, w_query=w_query, w_key=w_key, value_weight=value_weight, w_out=w_out, mlp_gain=mlp_gain, w_gate=w_gate, w_up=w_up, w_down=w_down, cotangent=cotangent)


NEG_BIG = -1e+30
EPSILON = 1e-05
THETA_BASE = 100000.0

@jax.custom_vjp
def low(v):
    return lax.optimization_barrier(v.astype(jnp.bfloat16)).astype(jnp.float32)

@jax.custom_vjp
def low_back(v):
    return v

def low_keep(v):
    return (low(v), None)

def low_pass(kept, grad):
    return (grad,)

def back_keep(v):
    return (v, None)

def back_low(kept, grad):
    return (low(grad),)
low.defvjp(low_keep, low_pass)
low_back.defvjp(back_keep, back_low)

def exact_dot(left_matrix, right_matrix):
    return jnp.dot(left_matrix, right_matrix, precision=lax.Precision.HIGHEST)

def rms_scale(features, gain_vector):
    factor = lax.rsqrt(lax.optimization_barrier(jnp.mean(features * features, axis=-1, keepdims=True)) + EPSILON)
    return features * factor * gain_vector

def rotary_tables(positions):
    half_width = HEAD_SIZE // 2
    frequency = THETA_BASE ** (-(jnp.arange(half_width, dtype=jnp.float32) * 2.0 / HEAD_SIZE))
    angles = positions[:, None] * frequency[None, :]
    return (jnp.cos(angles), jnp.sin(angles))

def rotate(features, cosine, sine_table):
    count_of_rows = features.shape[0]
    head_count = features.shape[1] // HEAD_SIZE
    shaped = features.reshape(count_of_rows, head_count, HEAD_SIZE)
    first_half = shaped[:, :, :HEAD_SIZE // 2]
    second_half = shaped[:, :, HEAD_SIZE // 2:]
    cos_part = cosine[:, None, :]
    sin_part = sine_table[:, None, :]
    joined = jnp.concatenate([first_half * cos_part - second_half * sin_part, second_half * cos_part + first_half * sin_part], axis=2)
    return joined.reshape(count_of_rows, head_count * HEAD_SIZE)

def token_starts(lengths_row, token_index):
    seq_ends = jnp.cumsum(lengths_row)
    passed = (seq_ends[None, :] <= token_index[:, None]).astype(jnp.int32)
    return lax.optimization_barrier(jnp.sum(passed * lengths_row[None, :], axis=1))

def visible(query_index, starts, key_index):
    return (key_index[None, :] <= query_index[:, None]) & (key_index[None, :] >= starts[:, None])

def group_forward(inputs, lengths_row, parameters):
    gain_one, query_proj, key_proj, value_proj, out_proj, gain_two, gate_weight, up_weight, down_weight = parameters
    count_of_rows = inputs.shape[0]
    group_width = QUERY_HEADS // KEY_VALUE_HEADS
    score_scale = 1.0 / math.sqrt(HEAD_SIZE)
    token_index = jnp.arange(count_of_rows, dtype=jnp.int32)
    starts = token_starts(lengths_row, token_index)
    cosine, sine_table = rotary_tables((token_index - starts).astype(jnp.float32))
    normed_one = low(rms_scale(inputs, gain_one))
    query_matrix = low(rotate(low_back(exact_dot(normed_one, query_proj)), cosine, sine_table))
    rows_of_key = low(rotate(low_back(exact_dot(normed_one, key_proj)), cosine, sine_table))
    rows_of_value = low(low_back(exact_dot(normed_one, value_proj)))
    heads_of_key = rows_of_key.reshape(count_of_rows, KEY_VALUE_HEADS, HEAD_SIZE)
    heads_of_value = rows_of_value.reshape(count_of_rows, KEY_VALUE_HEADS, HEAD_SIZE)
    rows_per_block = math.gcd(count_of_rows, 512)
    blocks_of_query = query_matrix.reshape(count_of_rows // rows_per_block, rows_per_block, KEY_VALUE_HEADS, group_width, HEAD_SIZE)

    def attend(block_item):
        block_number, query_part = block_item
        first_row = (block_number * rows_per_block).astype(jnp.int32)
        query_index = first_row + jnp.arange(rows_per_block, dtype=jnp.int32)
        query_start = lax.dynamic_slice_in_dim(starts, first_row, rows_per_block)
        visible_mask = visible(query_index, query_start, token_index)[:, None, None, :]
        scores = jnp.einsum('tkgd,skd->tkgs', query_part, heads_of_key, precision=lax.Precision.HIGHEST) * score_scale
        scores = low_back(scores)
        scores = jnp.where(visible_mask, scores, NEG_BIG)
        row_top = lax.optimization_barrier(jnp.max(scores, axis=3, keepdims=True))
        weights = jnp.exp(scores - row_top)
        normalizer = lax.optimization_barrier(jnp.sum(weights, axis=3))
        summed = low_back(jnp.einsum('tkgs,skd->tkgd', low(weights), heads_of_value, precision=lax.Precision.HIGHEST))
        return summed / normalizer[..., None]
    numbers = jnp.arange(count_of_rows // rows_per_block, dtype=jnp.int32)
    attention = lax.map(jax.checkpoint(attend), (numbers, blocks_of_query)).reshape(count_of_rows, QUERY_HEADS * HEAD_SIZE)
    attention = low(low_back(attention))
    middle = inputs + low_back(exact_dot(attention, out_proj))
    normed_two = low(rms_scale(middle, gain_two))
    gate_proj = low_back(exact_dot(normed_two, gate_weight))
    upward = low_back(exact_dot(normed_two, up_weight))
    product = low(jax.nn.silu(gate_proj) * upward)
    return middle + exact_dot(product, down_weight)

def reference(block_input, seq_lengths, attn_gain, w_query, w_key, value_weight, w_out, mlp_gain, w_gate, w_up, w_down, cotangent):
    parameters = (attn_gain.astype(jnp.float32), w_query.astype(jnp.float32), w_key.astype(jnp.float32), value_weight.astype(jnp.float32), w_out.astype(jnp.float32), mlp_gain.astype(jnp.float32), w_gate.astype(jnp.float32), w_up.astype(jnp.float32), w_down.astype(jnp.float32))
    group_inputs = block_input.astype(jnp.float32).reshape(N_FSDP, GROUP_TOK, MODEL_WIDTH)

    def whole_forward(inputs, weights_all):

        def one_group(block_item):
            return group_forward(block_item[0], block_item[1], weights_all)
        return lax.map(jax.checkpoint(one_group), (inputs, seq_lengths))
    outputs, pullback = jax.vjp(whole_forward, group_inputs, parameters)
    input_grad, param_grads = pullback(cotangent.astype(jnp.float32).reshape(N_FSDP, GROUP_TOK, MODEL_WIDTH))
    return (outputs.reshape(TOKENS, MODEL_WIDTH).astype(jnp.bfloat16), input_grad.reshape(TOKENS, MODEL_WIDTH), param_grads[0], param_grads[1], param_grads[2], param_grads[3], param_grads[4], param_grads[5], param_grads[6], param_grads[7], param_grads[8])
```

```python
import functools
import math

import jax
import jax.numpy as jnp
from jax import lax
from jax.experimental import pallas as pl
from jax.experimental.pallas import tpu as pltpu
from jax.sharding import PartitionSpec as P

HEAD_SIZE = 96
HALF = HEAD_SIZE // 2
LANES = 128
NEG_BIG = -1e30
EPSILON = 1e-05
THETA_BASE = 100000.0
SCALE = 1.0 / math.sqrt(HEAD_SIZE)
SCALE_LOG2 = SCALE * math.log2(math.e)
BF = jnp.bfloat16
F32 = jnp.float32


def dot(a, b, contract, out=F32):
    return lax.dot_general(
        a, b, ((contract[0], contract[1]), ((), ())), preferred_element_type=F32
    ).astype(out)


def shift(x, axis, by):
    n = lax.axis_size(axis)
    return lax.ppermute(x, axis, [(i, (i + by) % n) for i in range(n)])


def flip(x, axis, bit):
    n = lax.axis_size(axis)
    return lax.ppermute(x, axis, [(i, i ^ bit) for i in range(n)])


def spread(heads):
    row = jnp.arange(heads * HEAD_SIZE, dtype=jnp.int32)
    entry = row % HEAD_SIZE
    place = (row // HEAD_SIZE) * LANES + entry + jnp.where(entry >= HALF, LANES // 2 - HALF, 0)
    return (place[:, None] == jnp.arange(heads * LANES, dtype=jnp.int32)[None, :]).astype(BF)


def gather_weight(w, part_rows, dim, extra=None):
    nz, nc = lax.axis_size("fsdp"), lax.axis_size("ctx")
    z, c = lax.axis_index("fsdp"), lax.axis_index("ctx")
    rows, cols = w.shape
    if dim == 0:
        full = jnp.zeros((nz * rows, cols), w.dtype)
        place = lambda buf, piece, src, part: lax.dynamic_update_slice(
            buf, piece, (src * rows + part * part_rows, 0)
        )
        full = lax.dynamic_update_slice(full, w, (z * rows, 0))
    else:
        full = jnp.zeros((rows, nz * cols), w.dtype)
        place = lambda buf, piece, src, part: lax.dynamic_update_slice(
            buf, piece, (part * part_rows, src * cols)
        )
        full = lax.dynamic_update_slice(full, w, (0, z * cols))
    current = lax.dynamic_slice_in_dim(w, c * part_rows, part_rows, 0)
    if extra is not None:
        current = jnp.concatenate([current, extra], axis=0)
    extras = [extra]
    for step in range(1, nz):
        current = shift(current, "fsdp", 1)
        src = (z - step) % nz
        piece = current[:part_rows]
        full = place(full, piece, src, c)
        extras.append(current[part_rows:])
        for t in range(1, nc):
            other = shift(piece, "ctx", t)
            full = place(full, other, src, (c - t) % nc)
    return full, extras


def reduce_grad(g, dim):
    nz, nc = lax.axis_size("fsdp"), lax.axis_size("ctx")
    z, c = lax.axis_index("fsdp"), lax.axis_index("ctx")
    rows, cols = g.shape
    if dim == 0:
        shaped = g.reshape(nz, nc, rows // (nz * nc), cols)
        part = lambda p: lax.dynamic_index_in_dim(shaped, p, 1, keepdims=False)
        block = lambda h, b: lax.dynamic_index_in_dim(h, b, 0, keepdims=False)
    else:
        part = lambda p: lax.dynamic_slice_in_dim(g, p * (rows // nc), rows // nc, 0)
        block = lambda h, b: lax.dynamic_slice_in_dim(h, b * (cols // nz), cols // nz, 1)
    held = part(c).astype(F32)
    for t in range(1, nc):
        held = held + shift(part((c + t) % nc), "ctx", t).astype(F32)
    held = held.astype(BF)
    current = block(held, (z - 1) % nz)
    for step in range(1, nz):
        current = shift(current, "fsdp", 1)
        current = (current.astype(F32) + block(held, (z - 1 - step) % nz).astype(F32)).astype(BF)
    return join_parts(current).astype(F32)


def join_parts(own):
    nc, c = lax.axis_size("ctx"), lax.axis_index("ctx")
    if nc == 2:
        other = shift(own, "ctx", 1)
        return jnp.where(
            c == 0, jnp.concatenate([own, other], 0), jnp.concatenate([other, own], 0)
        )
    rows = own.shape[0]
    full = jnp.zeros((nc * rows, own.shape[1]), own.dtype)
    full = lax.dynamic_update_slice(full, own, (c * rows, 0))
    for t in range(1, nc):
        full = lax.dynamic_update_slice(full, shift(own, "ctx", t), (((c - t) % nc) * rows, 0))
    return full


def tp_sum(partial):
    if lax.axis_size("tp") != 4:
        return lax.psum(partial, "tp")
    h = lax.axis_index("tp") % 2
    half = partial.shape[0] // 2
    mine = lax.dynamic_slice_in_dim(partial, h * half, half, 0)
    theirs = lax.dynamic_slice_in_dim(partial, (1 - h) * half, half, 0)
    pair = (mine.astype(F32) + flip(theirs, "tp", 1).astype(F32)).astype(BF)
    total = (pair.astype(F32) + flip(pair, "tp", 2).astype(F32)).astype(BF)
    other = flip(total, "tp", 1)
    return jnp.where(
        h == 0, jnp.concatenate([total, other], 0), jnp.concatenate([other, total], 0)
    )


def tp_sum_rows(make, rows, pieces):
    size = rows // pieces
    return jnp.concatenate([tp_sum(make(i * size, size)) for i in range(pieces)], axis=0)


def qkv_kernel(hq, hk, x_ref, gain_ref, w_ref, cos_ref, sin_ref, sel_ref, normed_ref, q_ref, kv_ref):
    x = x_ref[...].astype(F32)
    r = lax.rsqrt(jnp.mean(x * x, axis=-1, keepdims=True) + EPSILON)
    normed = (x * r * gain_ref[...].astype(F32)).astype(BF)
    normed_ref[...] = normed
    acc = jnp.dot(normed, w_ref[...], preferred_element_type=F32)
    c, s = cos_ref[...], sin_ref[...]
    heads = []
    for i in range(hq + 2 * hk):
        v = acc[:, i * LANES : (i + 1) * LANES]
        if i < hq + hk:
            v = v * c + pltpu.roll(v, LANES // 2, 1) * s
        heads.append(v.astype(BF))
    q_ref[...] = jnp.concatenate(heads[:hq], axis=1)
    kv = jnp.concatenate(heads[hq:], axis=1)
    kv_ref[...] = jnp.dot(kv, sel_ref[...], preferred_element_type=F32).astype(BF)


def project(x, gain, w_pad, cos_t, sin_t, sel, hq, hk):
    rows, width = x.shape
    tile = math.gcd(rows, 256)
    wide = w_pad.shape[1]
    kv_cols = 2 * hk * HEAD_SIZE
    return pl.pallas_call(
        functools.partial(qkv_kernel, hq, hk),
        grid=(rows // tile,),
        in_specs=[
            pl.BlockSpec((tile, width), lambda i: (i, 0)),
            pl.BlockSpec((1, width), lambda i: (0, 0)),
            pl.BlockSpec((width, wide), lambda i: (0, 0)),
            pl.BlockSpec((tile, LANES), lambda i: (i, 0)),
            pl.BlockSpec((tile, LANES), lambda i: (i, 0)),
            pl.BlockSpec((2 * hk * LANES, kv_cols), lambda i: (0, 0)),
        ],
        out_specs=[
            pl.BlockSpec((tile, width), lambda i: (i, 0)),
            pl.BlockSpec((tile, hq * LANES), lambda i: (i, 0)),
            pl.BlockSpec((tile, kv_cols), lambda i: (i, 0)),
        ],
        out_shape=[
            jax.ShapeDtypeStruct((rows, width), BF),
            jax.ShapeDtypeStruct((rows, hq * LANES), BF),
            jax.ShapeDtypeStruct((rows, kv_cols), BF),
        ],
        cost_estimate=pl.CostEstimate(
            flops=2 * rows * width * wide, bytes_accessed=12 * 2**20, transcendentals=0
        ),
        name="qkv",
    )(x, gain, w_pad, cos_t, sin_t, sel)


def attend_kernel(bq, bk, meta_ref, q_ref, k_ref, v_ref, st_ref, o_ref, lse_ref):
    i = pl.program_id(1)
    q = jnp.concatenate([q_ref[:, :LANES], q_ref[:, LANES:]], axis=0)
    first = meta_ref[0] + i * bq
    at = first + lax.broadcasted_iota(jnp.int32, (1, bq), 1)
    at = jnp.concatenate([at, at], axis=1)
    st = jnp.concatenate([st_ref[...], st_ref[...]], axis=1)
    low = meta_ref[1 + i] // bk
    high = (first + bq - 1) // bk

    def step(j, carry):
        top, total, acc = carry
        rows = pl.ds(pl.multiple_of(j * bk, bk), bk)
        s = dot(k_ref[rows, :], q, ((1,), (1,))) * SCALE_LOG2
        key = j * bk + lax.broadcasted_iota(jnp.int32, (bk, 1), 0)
        s = jnp.where((key <= at) & (key >= st), s, NEG_BIG)
        new = jnp.maximum(top, jnp.max(s, axis=0, keepdims=True))
        p = jnp.exp2(s - new)
        scale = jnp.exp2(top - new)
        total = total * scale + jnp.sum(p, axis=0, keepdims=True)
        acc = acc * scale + dot(v_ref[rows, :], p.astype(BF), ((0,), (0,)))
        return new, total, acc

    top, total, acc = lax.fori_loop(
        low,
        high + 1,
        step,
        (
            jnp.full((1, 2 * bq), NEG_BIG, F32),
            jnp.zeros((1, 2 * bq), F32),
            jnp.zeros((LANES, 2 * bq), F32),
        ),
    )
    out = (acc / total).T.astype(BF)
    o_ref[...] = jnp.concatenate([out[:bq], out[bq:]], axis=1)
    lse = top + jnp.log2(total)
    lse_ref[...] = jnp.concatenate([lse[:, :bq], lse[:, bq:]], axis=0)[None]


def attend(meta, q, k, v, starts, bq, bk):
    rows, kv_heads = q.shape[0], k.shape[1] // LANES
    keys = k.shape[0]
    pairs = q.shape[1] // (kv_heads * LANES)
    assert pairs == 2
    return pl.pallas_call(
        functools.partial(attend_kernel, bq, bk),
        grid_spec=pltpu.PrefetchScalarGridSpec(
            num_scalar_prefetch=1,
            grid=(kv_heads, rows // bq),
            in_specs=[
                pl.BlockSpec((bq, 2 * LANES), lambda g, i, m: (i, g)),
                pl.BlockSpec((keys, LANES), lambda g, i, m: (0, g)),
                pl.BlockSpec((keys, LANES), lambda g, i, m: (0, g)),
                pl.BlockSpec((1, bq), lambda g, i, m: (0, i)),
            ],
            out_specs=[
                pl.BlockSpec((bq, 2 * LANES), lambda g, i, m: (i, g)),
                pl.BlockSpec((1, 2, bq), lambda g, i, m: (g, 0, i)),
            ],
        ),
        out_shape=[
            jax.ShapeDtypeStruct(q.shape, BF),
            jax.ShapeDtypeStruct((kv_heads, 2, rows), F32),
        ],
        cost_estimate=pl.CostEstimate(
            flops=16 * rows * 1024 * LANES, bytes_accessed=6 * 2**20, transcendentals=4 * rows * 1024
        ),
        name="attend",
    )(meta, q, k, v, starts)


def attend_back_kernel(
    bq, bk, meta_ref, q_ref, k_ref, v_ref, st_ref, do_ref, o_ref, lse_ref, cos_ref, sin_ref,
    dq_ref, dk_ref, dv_ref, dk_acc, dv_acc,
):
    i = pl.program_id(1)

    @pl.when(i == 0)
    def _():
        dk_acc[...] = jnp.zeros_like(dk_acc)
        dv_acc[...] = jnp.zeros_like(dv_acc)

    stack = lambda ref: jnp.concatenate([ref[:, :LANES], ref[:, LANES:]], axis=0)
    q, do, o = stack(q_ref), stack(do_ref), stack(o_ref)
    delta = jnp.sum((do.astype(F32) * o.astype(F32)).T, axis=0, keepdims=True)
    lse = jnp.concatenate([lse_ref[0, 0:1, :], lse_ref[0, 1:2, :]], axis=1)
    first = meta_ref[0] + i * bq
    at = first + lax.broadcasted_iota(jnp.int32, (1, bq), 1)
    at = jnp.concatenate([at, at], axis=1)
    st = jnp.concatenate([st_ref[...], st_ref[...]], axis=1)
    low = meta_ref[1 + i] // bk
    high = (first + bq - 1) // bk

    def step(j, acc):
        rows = pl.ds(pl.multiple_of(j * bk, bk), bk)
        k = k_ref[rows, :]
        s = dot(k, q, ((1,), (1,))) * SCALE_LOG2
        key = j * bk + lax.broadcasted_iota(jnp.int32, (bk, 1), 0)
        p = jnp.where((key <= at) & (key >= st), jnp.exp2(s - lse), 0.0)
        dp = dot(v_ref[rows, :], do, ((1,), (1,)))
        ds = (p * (dp - delta)).astype(BF)
        dv_acc[rows, :] += dot(p.astype(BF), do, ((1,), (0,)))
        dk_acc[rows, :] += dot(ds, q, ((1,), (0,)))
        return acc + dot(k, ds, ((0,), (0,)))

    acc = lax.fori_loop(low, high + 1, step, jnp.zeros((LANES, 2 * bq), F32))
    dq = acc.T * SCALE
    c, s = cos_ref[...], sin_ref[...]
    back = lambda v: (v * c - pltpu.roll(v, LANES // 2, 1) * s).astype(BF)
    dq_ref[...] = jnp.concatenate([back(dq[:bq]), back(dq[bq:])], axis=1)

    @pl.when(i == pl.num_programs(1) - 1)
    def _():
        dk_ref[...] = (dk_acc[...] * SCALE).astype(BF)
        dv_ref[...] = dv_acc[...].astype(BF)


def attend_back(meta, q, k, v, starts, do, o, lse, cos_t, sin_t, bq, bk):
    rows, kv_heads = q.shape[0], k.shape[1] // LANES
    keys = k.shape[0]
    block = pl.BlockSpec((bq, 2 * LANES), lambda g, i, m: (i, g))
    whole = pl.BlockSpec((keys, LANES), lambda g, i, m: (0, g))
    table = pl.BlockSpec((bq, LANES), lambda g, i, m: (i, 0))
    return pl.pallas_call(
        functools.partial(attend_back_kernel, bq, bk),
        grid_spec=pltpu.PrefetchScalarGridSpec(
            num_scalar_prefetch=1,
            grid=(kv_heads, rows // bq),
            in_specs=[
                block,
                whole,
                whole,
                pl.BlockSpec((1, bq), lambda g, i, m: (0, i)),
                block,
                block,
                pl.BlockSpec((1, 2, bq), lambda g, i, m: (g, 0, i)),
                table,
                table,
            ],
            out_specs=[block, whole, whole],
            scratch_shapes=[pltpu.VMEM((keys, LANES), F32), pltpu.VMEM((keys, LANES), F32)],
        ),
        out_shape=[
            jax.ShapeDtypeStruct(q.shape, BF),
            jax.ShapeDtypeStruct(k.shape, BF),
            jax.ShapeDtypeStruct(k.shape, BF),
        ],
        cost_estimate=pl.CostEstimate(
            flops=40 * rows * 1024 * LANES, bytes_accessed=10 * 2**20, transcendentals=4 * rows * 1024
        ),
        name="attend_back",
    )(meta, q, k, v, starts, do, o, lse, cos_t, sin_t)


def finish_kernel(hq, hk, got, *refs):
    dq_ref, cos_ref, sin_ref, selq_ref, selk_ref = refs[:5]
    dk = refs[5][...].astype(F32)
    dv = refs[6][...].astype(F32)
    for t in range(got):
        part = refs[7 + t][...].astype(F32)
        dk = dk + part[:, : hk * LANES]
        dv = dv + part[:, hk * LANES :]
    out_ref = refs[7 + got]
    c, s = cos_ref[...], sin_ref[...]
    heads = []
    for i in range(hk):
        x = dk[:, i * LANES : (i + 1) * LANES]
        heads.append((x * c - pltpu.roll(x, LANES // 2, 1) * s).astype(BF))
    kv = jnp.concatenate(heads + [dv.astype(BF)], axis=1)
    out_ref[...] = jnp.concatenate(
        [
            jnp.dot(dq_ref[...], selq_ref[...], preferred_element_type=F32).astype(BF),
            jnp.dot(kv, selk_ref[...], preferred_element_type=F32).astype(BF),
        ],
        axis=1,
    )


def finish(dq, cos_t, sin_t, selq, selk, dk, dv, received, hq, hk):
    rows = dq.shape[0]
    tile = math.gcd(rows, 256)
    cols = (hq + 2 * hk) * HEAD_SIZE
    by_row = lambda a: pl.BlockSpec((tile, a.shape[1]), lambda i: (i, 0))
    whole = lambda a: pl.BlockSpec(a.shape, lambda i: (0, 0))
    return pl.pallas_call(
        functools.partial(finish_kernel, hq, hk, len(received)),
        grid=(rows // tile,),
        in_specs=[by_row(dq), by_row(cos_t), by_row(sin_t), whole(selq), whole(selk), by_row(dk), by_row(dv)]
        + [by_row(a) for a in received],
        out_specs=pl.BlockSpec((tile, cols), lambda i: (i, 0)),
        out_shape=jax.ShapeDtypeStruct((rows, cols), BF),
        cost_estimate=pl.CostEstimate(
            flops=4 * rows * 512 * 384, bytes_accessed=6 * 2**20, transcendentals=0
        ),
        name="finish",
    )(dq, cos_t, sin_t, selq, selk, dk, dv, *received)


def norm_back(grad, value, gain_f, r):
    u = grad * gain_f
    mean = jnp.mean(u * value, axis=-1, keepdims=True)
    return r * u - value * (r * r * r) * mean


def per_device(
    block_input, seq_lengths, attn_gain, w_query, w_key, value_weight, w_out, mlp_gain, w_gate, w_up, w_down, cotangent
):
    nz, nc = lax.axis_size("fsdp"), lax.axis_size("ctx")
    z, c = lax.axis_index("fsdp"), lax.axis_index("ctx")
    rows, width = block_input.shape
    hq, hk = w_query.shape[1] // HEAD_SIZE, w_key.shape[1] // HEAD_SIZE
    ff = w_gate.shape[1]
    shard = w_query.shape[0]

    w_qkv = jnp.concatenate([w_query, w_key, value_weight], axis=1)
    gains = jnp.concatenate([attn_gain, mlp_gain])
    qkv_cols = w_qkv.shape[1]
    gain_rows = 16
    extra = jnp.pad(gains, (0, gain_rows * qkv_cols - gains.shape[0])).reshape(gain_rows, qkv_cols)
    qkv_full, extras = gather_weight(w_qkv, shard // nc, 0, extra)
    gain_pieces = jnp.stack([e.reshape(-1)[: 2 * shard] for e in extras])
    gain_pieces = jnp.take(gain_pieces, (z - jnp.arange(nz)) % nz, axis=0)
    gain_one = gain_pieces[:, :shard].reshape(1, width)
    gain_two = gain_pieces[:, shard:].reshape(1, width)
    out_full, _ = gather_weight(w_out, w_out.shape[0] // nc, 1)
    gu_full, _ = gather_weight(jnp.concatenate([w_gate, w_up], axis=1), shard // nc, 0)
    down_full, _ = gather_weight(w_down, w_down.shape[0] // nc, 1)

    first_token = c * rows
    at = first_token + jnp.arange(rows, dtype=jnp.int32)
    ends = jnp.cumsum(seq_lengths[0])
    passed = (ends[None, :] <= at[:, None]).astype(jnp.int32)
    starts = jnp.sum(passed * seq_lengths[0][None, :], axis=1)
    lane = jnp.arange(LANES, dtype=jnp.int32)
    index = (lane % (LANES // 2)).astype(F32)
    frequency = THETA_BASE ** (-(index * 2.0 / HEAD_SIZE))
    angle = (at - starts).astype(F32)[:, None] * frequency[None, :]
    cos_t = jnp.cos(angle)
    sin_t = jnp.sin(angle) * jnp.where(lane < LANES // 2, -1.0, 1.0)[None, :]
    bq, bk = math.gcd(rows, 256), math.gcd(rows, 512)
    meta = jnp.concatenate([first_token.reshape(1).astype(jnp.int32), starts[::bq]])
    starts_row = starts.reshape(1, rows)

    selq, selk = spread(hq), spread(2 * hk)
    qcols = hq * HEAD_SIZE
    w_pad = jnp.concatenate(
        [
            dot(qkv_full[:, :qcols], selq, ((1,), (0,)), BF),
            dot(qkv_full[:, qcols:], selk, ((1,), (0,)), BF),
        ],
        axis=1,
    )
    normed_one, q, kv = project(block_input, gain_one, w_pad, cos_t, sin_t, selk.T, hq, hk)
    kv_all = jnp.zeros((nc * rows, kv.shape[1]), BF)
    kv_all = lax.dynamic_update_slice(kv_all, kv, (c * rows, 0))
    for t in range(1, nc):
        piece = lax.ppermute(kv, "ctx", [(i, i + t) for i in range(nc - t)])
        kv_all = lax.dynamic_update_slice(kv_all, piece, (((c - t) % nc) * rows, 0))
    kcols = hk * HEAD_SIZE
    selh = spread(hk)
    k_all = dot(kv_all[:, :kcols], selh, ((1,), (0,)), BF)
    v_all = dot(kv_all[:, kcols:], selh, ((1,), (0,)), BF)
    attention, lse = attend(meta, q, k_all, v_all, starts_row, bq, bk)
    out_pad = dot(selq, out_full, ((0,), (0,)), BF)
    inputs = block_input.astype(F32)
    branch = tp_sum_rows(
        lambda a, n: dot(attention[a : a + n], out_pad, ((1,), (0,)), BF), rows, 2
    )

    middle = inputs + branch.astype(F32)
    gain_two_f = gain_two.astype(F32)
    r_two = lax.rsqrt(jnp.mean(middle * middle, axis=-1, keepdims=True) + EPSILON)
    normed_two = (middle * r_two * gain_two_f).astype(BF)
    product_grad = dot(cotangent, down_full, ((1,), (1,)))
    gate_up = dot(normed_two, gu_full, ((1,), (0,)))
    gate_proj, upward = gate_up[:, :ff], gate_up[:, ff:]
    sig = jax.nn.sigmoid(gate_proj)
    product = (gate_proj * sig * upward).astype(BF)
    gu_grad = jnp.concatenate(
        [
            (product_grad * upward * sig * (1.0 + gate_proj * (1.0 - sig))).astype(BF),
            (product_grad * gate_proj * sig).astype(BF),
        ],
        axis=1,
    )
    normed_two_grad = tp_sum_rows(
        lambda a, n: dot(gu_grad[a : a + n], gu_full, ((1,), (1,)), BF), rows, 2
    ).astype(F32)
    down_grad = reduce_grad(dot(product, cotangent, ((0,), (0,)), BF), 1)
    gate_grad = reduce_grad(dot(normed_two, gu_grad[:, :ff], ((0,), (0,)), BF), 0)
    up_grad = reduce_grad(dot(normed_two, gu_grad[:, ff:], ((0,), (0,)), BF), 0)
    mlp = tp_sum_rows(
        lambda a, n: dot(product[a : a + n], down_full, ((1,), (0,)), BF), rows, 2
    )
    block_output = (middle + mlp.astype(F32)).astype(BF)
    gain_two_part = jnp.sum(normed_two_grad * middle * r_two, axis=0)
    middle_grad = cotangent.astype(F32) + norm_back(normed_two_grad, middle, gain_two_f, r_two)

    branch_grad = middle_grad.astype(BF)
    attention_grad = dot(branch_grad, out_pad, ((1,), (1,)), BF)
    dq, dk, dv = attend_back(
        meta, q, k_all, v_all, starts_row, attention_grad, attention, lse, cos_t, sin_t, bq, bk
    )
    dkv = jnp.concatenate([dk, dv], axis=1)
    received = []
    for t in range(1, nc):
        piece = lax.dynamic_slice_in_dim(dkv, ((c - t) % nc) * rows, rows, 0)
        received.append(lax.ppermute(piece, "ctx", [(i + t, i) for i in range(nc - t)]))
    own_k = lax.dynamic_slice_in_dim(dk, c * rows, rows, 0)
    own_v = lax.dynamic_slice_in_dim(dv, c * rows, rows, 0)
    compact = dot(attention, selq, ((1,), (1,)), BF)
    out_grad = reduce_grad(dot(compact, branch_grad, ((0,), (0,)), BF), 1)
    dqkv = finish(dq, cos_t, sin_t, selq.T, selk.T, own_k, own_v, received, hq, hk)
    qkv_grad = reduce_grad(dot(normed_one, dqkv, ((0,), (0,)), BF), 0)
    partial = dot(dqkv, qkv_full, ((1,), (1,)))
    gain_one_f = gain_one.astype(F32)
    r_one = lax.rsqrt(jnp.mean(inputs * inputs, axis=-1, keepdims=True) + EPSILON)
    gain_one_part = jnp.sum(partial * (inputs * r_one), axis=0)
    size = rows // 2
    partial = partial.astype(BF)
    normed_one_grad = jnp.concatenate(
        [tp_sum(partial[i * size : (i + 1) * size]) for i in range(2)], axis=0
    ).astype(F32)
    input_grad = middle_grad + norm_back(normed_one_grad, inputs, gain_one_f, r_one)

    gain_two_part = jnp.where(lax.axis_index("tp") == 0, gain_two_part, 0.0)
    both = jnp.stack([gain_one_part, gain_two_part])
    n = lax.axis_size("tp")
    bit = 1
    while bit < n:
        both = both + flip(both, "tp", bit)
        bit *= 2
    ranks = [(c - t) % nc for t in range(nc)]
    seen = jnp.zeros((nc,) + both.shape, F32)
    for t in range(nc):
        seen = lax.dynamic_update_slice(
            seen, (shift(both, "ctx", t) if t else both)[None], (ranks[t], 0, 0)
        )
    both = jnp.sum(seen, axis=0)
    piece = lambda b: lax.dynamic_slice_in_dim(both, b * shard, shard, 1)
    owned = piece(z)
    for t in range(1, nz):
        owned = owned + shift(piece((z + t) % nz), "fsdp", t)

    kv_width = w_key.shape[1]
    return (
        block_output,
        input_grad,
        owned[0],
        qkv_grad[:, :qcols],
        qkv_grad[:, qcols : qcols + kv_width],
        qkv_grad[:, qcols + kv_width :],
        out_grad,
        owned[1],
        gate_grad,
        up_grad,
        down_grad,
    )


def solution(mesh):
    in_specs = (
        P(("fsdp", "ctx"), None),
        P("fsdp", None),
        P("fsdp"),
        P("fsdp", "tp"),
        P("fsdp", "tp"),
        P("fsdp", "tp"),
        P("tp", "fsdp"),
        P("fsdp"),
        P("fsdp", "tp"),
        P("fsdp", "tp"),
        P("tp", "fsdp"),
        P(("fsdp", "ctx"), None),
    )
    out_specs = (
        P(("fsdp", "ctx"), None),
        P(("fsdp", "ctx"), None),
        P("fsdp"),
        P("fsdp", "tp"),
        P("fsdp", "tp"),
        P("fsdp", "tp"),
        P("tp", "fsdp"),
        P("fsdp"),
        P("fsdp", "tp"),
        P("fsdp", "tp"),
        P("tp", "fsdp"),
    )
    return jax.shard_map(
        per_device, mesh=mesh, in_specs=in_specs, out_specs=out_specs, check_vma=False
    )
```
